32 devices in a mesh: dp: 8 (over z, x), cent: 4 (over y, core).
Axes of the slice: x: 2, y: 2, z: 4, core: 2. Of those that a mesh axis runs over, the one named last changes fastest.
Arguments:
- points: float32 [16384, 512], P('dp'), may hold values from -30 to 30
- centroids: float32 [16384, 512], P('cent'), may hold values from -5 to 5
Outputs:
- new_centroids: float32 [16384, 512], P('cent')
The draws below stay inside these ranges and needn't reach their ends.
All inputs are finite; a program needn't handle non-finite values.
Results may differ from the reference program's by a relative error of at most 0.0061.
Values sent between devices are 32-bit elements; how exact they have to be, the bound alone decides.
A program may use at most 128 MiB of HBM per device.

```python
import jax
import jax.numpy as jnp
from jax import lax

D = 512
K = 16384
POINTS = 16384


def shared_centroids(key):
    base = jnp.clip(jax.random.normal(jax.random.fold_in(key, 11), (K, D), jnp.float32), -5.0, 5.0)
    return base


def draw_centroids(key, part):
    return shared_centroids(key)


def draw_points(key, part):
    base = jnp.clip(jax.random.normal(jax.random.fold_in(key, 12), (POINTS, D), jnp.float32), -6.0, 6.0)
    cents = shared_centroids(key)
    picks = 2 * jax.random.randint(jax.random.fold_in(key, 15), (POINTS,), 0, K // 2)
    level = jax.random.randint(jax.random.fold_in(key, 16), (POINTS,), 0, 4).astype(jnp.float32)
    target = 110.0 + 60.0 * level
    factor = 0.5 * (target / jnp.sqrt(jnp.float32(D)) + 1.0)
    aligned = factor[:, None] * cents[picks]
    chosen = jnp.arange(POINTS) % 64 == 0
    base = jnp.where(chosen[:, None], aligned, base)
    return jnp.clip(base, -30.0, 30.0)


def setup_inputs(seed: int = 0) -> dict:
    splits = jax.random.split(jax.random.key(seed), 3)
    points = draw_points(jax.random.fold_in(splits[2], 71), 0)
    centroids = draw_centroids(jax.random.fold_in(splits[2], 71), 0)
    return {"points": points, "centroids": centroids}


def reference(points, centroids):
    cent_half = centroids.astype(jnp.bfloat16)
    sq_norm = lax.optimization_barrier(jnp.sum(centroids * centroids, axis=1))
    scale = 1.0 / jnp.sqrt(jnp.float32(D))
    block_rows = min(1024, POINTS)
    blocks = points.reshape(POINTS // block_rows, block_rows, D)

    def step(carry, block):
        weighted, counts = carry
        point_half = block.astype(jnp.bfloat16)
        inner = jnp.dot(point_half, cent_half.T, preferred_element_type=jnp.float32)
        logit = (2.0 * inner - sq_norm[None, :]) * scale
        top = lax.optimization_barrier(jnp.max(logit, axis=1, keepdims=True))
        expo = jnp.exp(logit - top)
        total = lax.optimization_barrier(jnp.sum(expo, axis=1, keepdims=True))
        resp = (expo / total).astype(jnp.bfloat16)
        weighted = weighted + jnp.dot(resp.T, point_half, preferred_element_type=jnp.float32)
        counts = counts + lax.optimization_barrier(jnp.sum(resp.astype(jnp.float32), axis=0))
        return ((weighted, counts), None)
    start = (jnp.zeros((K, D), jnp.float32), jnp.zeros((K,), jnp.float32))
    (weighted, counts), unused = lax.scan(step, start, blocks)
    return (weighted + centroids) / (counts + 1.0)[:, None]
```

```python
import functools

import jax
import jax.numpy as jnp
from jax import lax
from jax.experimental import pallas as pl
from jax.experimental.pallas import tpu as pltpu
from jax.sharding import PartitionSpec as P

MESH = pl.DeviceIdType.MESH
LANES = 128
LAG = 3
BACK = 2
EVERY = 2
LATE = 2
LOG2E = 1.4426950408889634


def kernel(
    ndp, ncent, geo, pts_ref, cen_ref, out_ref,
    pbuf, ph, cenf, cenh, bias, ybuf, expo, stats, scale_ref,
    part, low, high, cnt_part, cnt_low, cnt_high, cnt_col,
    load_sem, pt_recv, px_send, py_send, pc_send, st_send, st_recv,
    sum_send, low_recv, high_recv, cnt_send, cl_recv, ch_recv,
    up_send, down_send, res_recv, xp_send, xp_recv,
):
    rows, half, pb, sub, kb, mb, chunk = geo
    width = pts_ref.shape[1]
    chain = ndp // 2
    last = chain - 1
    root0, root1 = last // 2, last - last // 2
    dirs = half // 2
    count = dirs // chunk
    share = rows // ncent
    seg = pb // ncent
    per = seg // sub
    nsub = share // sub
    nblk = rows // pb
    hp = pb // LANES
    first = nblk - LATE
    upc = mb // chunk
    units = dirs // mb

    me = lax.axis_index("dp")
    cent = lax.axis_index("cent")
    z, x = me // 2, lax.rem(me, 2)
    core, yy = lax.rem(cent, 2), cent // 2
    other = z * 2 + (1 - x)
    mate = yy * 2 + (1 - core)
    mine = x * ncent + cent
    group = 2 * ncent

    def remote(src, dst, send, got, dp, ce):
        return pltpu.make_async_remote_copy(
            src_ref=src, dst_ref=dst, send_sem=send, recv_sem=got,
            device_id=(dp, ce), device_id_type=MESH,
        )

    def owned(owner):
        return pl.ds(pl.multiple_of(owner * share, share), share)

    loads = []
    for o in range(ncent):
        owner = lax.rem(cent + o, ncent)
        loads.append(
            pltpu.make_async_copy(pts_ref.at[owned(owner)], pbuf.at[owned(owner)], load_sem.at[o])
        )
    load_c = pltpu.make_async_copy(
        cen_ref.at[pl.ds(pl.multiple_of(x * half, half), half)], cenf, load_sem.at[ncent]
    )
    for copy in loads:
        copy.start()
    load_c.start()

    barrier = pltpu.get_barrier_semaphore()
    for o in range(1, group):
        peer = lax.rem(mine + o, group)
        pl.semaphore_signal(
            barrier, inc=1, device_id=(z * 2 + peer // ncent, lax.rem(peer, ncent)),
            device_id_type=MESH,
        )

    @pl.when(z > 0)
    def _():
        pl.semaphore_signal(barrier, inc=1, device_id=(me - 2, cent), device_id_type=MESH)

    @pl.when(z < last)
    def _():
        pl.semaphore_signal(barrier, inc=1, device_id=(me + 2, cent), device_id_type=MESH)

    ends = jnp.where(z > 0, 1, 0) + jnp.where(z < last, 1, 0)
    pl.semaphore_wait(barrier, group - 1 + ends)
    loads[0].wait()

    def span(side, owner, j):
        return pl.ds(pl.multiple_of(side * rows + owner * share + j * sub, sub), sub)

    for j in range(nsub):
        remote(
            pbuf.at[span(0, cent, j)], pbuf.at[span(1, cent, j)],
            px_send, pt_recv.at[cent * nsub + j], other, cent,
        ).start()
    for copy in loads[1:]:
        copy.wait()
    load_c.wait()

    root = jnp.float32(1.0) / jnp.sqrt(jnp.float32(width))
    gain = 2.0 * root * LOG2E
    norm_gain = root * LOG2E

    def prepare(k, carry):
        at = pl.ds(pl.multiple_of(k * mb, mb), mb)
        c = cenf[at, :]
        cenh[at, :] = c.astype(jnp.bfloat16)
        bias[at, :] = jnp.broadcast_to(
            jnp.sum(c * c, axis=1, keepdims=True) * norm_gain, (mb, LANES)
        )
        return carry

    lax.fori_loop(0, half // mb, prepare, 0)

    def block(side, b):
        pv = jnp.concatenate([
            pbuf[pl.ds(pl.multiple_of(side * rows + o * share + b * seg, seg), seg), :]
            for o in range(ncent)
        ], axis=0).astype(jnp.bfloat16)
        origin = lax.rem(x + side, 2)
        cols = pl.ds(pl.multiple_of(b * 2 * pb + origin * pb, pb), pb)
        ph[cols, :] = pv

        def logits(k, top):
            at = pl.ds(pl.multiple_of(k * kb, kb), kb)
            inner = lax.dot_general(
                cenh[at, :], pv, (((1,), (1,)), ((), ())), preferred_element_type=jnp.float32
            )
            v = bias[at, :]
            y = inner * gain - jnp.concatenate([v] * hp, axis=1)
            ybuf[at, :] = y
            return jnp.maximum(top, jnp.max(y, axis=0, keepdims=True))

        top = lax.fori_loop(
            0, half // kb, logits, jnp.full((1, pb), -jnp.inf, jnp.float32), unroll=True
        )

        def powers(k, total):
            at = pl.ds(pl.multiple_of(k * kb, kb), kb)
            e = jnp.exp2(ybuf[at, :] - top)
            expo[at, cols] = e.astype(jnp.bfloat16)
            return total + jnp.sum(e, axis=0, keepdims=True)

        total = lax.fori_loop(0, half // kb, powers, jnp.zeros((1, pb), jnp.float32), unroll=True)
        for h in range(hp):
            lane = slice(h * LANES, (h + 1) * LANES)
            stats[mine, b, pl.ds(origin * hp + h, 1), :] = top[:, lane]
            stats[mine, b, pl.ds((2 + origin) * hp + h, 1), :] = total[:, lane]

    ny = ncent // 2
    same = [lax.rem(yy + d, ny) * 2 + core for d in range(1, ny)]
    cross = [lax.rem(yy + d, ny) * 2 + (1 - core) for d in range(1, ny)]

    def arrived(owner, j):
        at = pbuf.at[span(1, owner, j)]
        remote(at, at, px_send, pt_recv.at[owner * nsub + j], other, cent).wait_recv()

    def forward(owner, j, ce, sem):
        at = pbuf.at[span(1, owner, j)]
        remote(at, at, sem, pt_recv.at[owner * nsub + j], me, ce).start()

    def relay_x(j, carry):
        arrived(cent, j)
        for i, d in enumerate(same):
            forward(cent, j, d, py_send.at[i])
        forward(cent, j, mate, pc_send.at[0])
        return carry

    def relay_y(j, carry):
        for i, d in enumerate(same):
            arrived(d, j)
            forward(d, j, mate, pc_send.at[i + 1])
        return carry

    def x_until(k):
        own = jnp.minimum(k + 1, nblk)
        return jnp.minimum(nsub, jnp.maximum(own, jnp.where(k >= nblk, per * (k - nblk + 3) + 1, 0)))

    def y_until(k):
        own = jnp.clip(k - 2, 0, nblk - 3)
        return jnp.minimum(nsub, jnp.maximum(own, jnp.where(k >= nblk, per * (k - nblk + 2) + 1, 0)))

    def stat_copies(late):
        part_of = pl.ds(first, LATE) if late else pl.ds(0, first)
        copies = []
        for o in range(1, group):
            peer = lax.rem(mine + o, group)
            at = stats.at[mine, part_of]
            copies.append(remote(
                at, at, st_send.at[late * group + o], st_recv.at[late * group + mine],
                z * 2 + peer // ncent, lax.rem(peer, ncent),
            ))
        return copies

    def stat_wait(late):
        part_of = pl.ds(first, LATE) if late else pl.ds(0, first)
        for o in range(1, group):
            peer = lax.rem(mine + o, group)
            at = stats.at[peer, part_of]
            remote(
                at, at, st_send.at[late * group + o], st_recv.at[late * group + peer], other, cent
            ).wait_recv()

    def step(k, carry):
        side, b = k // nblk, lax.rem(k, nblk)

        @pl.when(side > 0)
        def _():
            def ready(j, c):
                arrived(mate, j)
                for d in cross:
                    arrived(d, j)
                return c

            lax.fori_loop(b * per, b * per + per, ready, 0)

        block(side, b)
        lax.fori_loop(x_until(k - 1), x_until(k), relay_x, 0)

        @pl.when(k == nblk + first - 1)
        def _():
            for copy in stat_copies(0):
                copy.start()

        lax.fori_loop(y_until(k - 1), y_until(k), relay_y, 0)
        return carry

    lax.fori_loop(0, 2 * nblk, step, 0)
    for copy in stat_copies(1):
        copy.start()

    def settle(late):
        lo, hi = (first, nblk) if late else (0, first)
        stat_wait(late)
        peak = stats[0, lo:hi, 0:2 * hp, :]
        for s in range(1, group):
            peak = jnp.maximum(peak, stats[s, lo:hi, 0:2 * hp, :])
        summed = jnp.zeros((hi - lo, 2 * hp, LANES), jnp.float32)
        for s in range(group):
            summed = summed + stats[s, lo:hi, 2 * hp:, :] * jnp.exp2(stats[s, lo:hi, 0:2 * hp, :] - peak)
        scale_ref[lo:hi] = jnp.exp2(stats[mine, lo:hi, 0:2 * hp, :] - peak) / summed

    def weigh(d, j, lo, hi):
        at = pl.ds(pl.multiple_of(d * dirs + j * mb, mb), mb)
        slot = d * units + j

        def rescale(q, acc):
            cols = pl.ds(pl.multiple_of(q * LANES, LANES), LANES)
            r = expo[at, cols].astype(jnp.float32) * scale_ref[q // (2 * hp), pl.ds(lax.rem(q, 2 * hp), 1), :]
            r = r.astype(jnp.bfloat16)
            expo[at, cols] = r
            return acc + r.astype(jnp.float32)

        scale = 2 * hp
        acc = lax.fori_loop(
            lo * scale, hi * scale, rescale, jnp.zeros((mb, LANES), jnp.float32), unroll=True
        )
        lines = [
            jnp.sum(acc[h * LANES:(h + 1) * LANES, :].T, axis=0, keepdims=True)
            for h in range(mb // LANES)
        ]
        lines = jnp.concatenate(lines * (8 // len(lines)), axis=0)
        pts = slice(lo * 2 * pb, hi * 2 * pb)
        dots = jnp.dot(expo[at, pts], ph[pts, :], preferred_element_type=jnp.float32)
        if lo == 0:
            cnt_part[slot] = lines
            part[at, :] = dots
        else:
            cnt_part[slot] = cnt_part[slot] + lines
            part[at, :] = part[at, :] + dots

    settle(0)
    lax.fori_loop(0, 2, lambda d, c: (weigh(d, 0, 0, first), c)[1], 0)
    settle(1)
    lax.fori_loop(0, 2, lambda d, c: (weigh(d, 0, first, nblk), c)[1], 0)

    flip = jnp.where(z < chain // 2, 0, 1)

    def crows(d, i):
        return pl.ds(pl.multiple_of(d * dirs + i * chunk, chunk), chunk)

    def orows(d, i):
        return pl.ds(pl.multiple_of(x * half + d * dirs + i * chunk, chunk), chunk)

    def pass_on(d, i, src, dst, got, cnt, cnt_dst, cnt_got, dp):
        at = crows(d, i)
        remote(src.at[at], dst.at[at], sum_send.at[d], got.at[d * count + i], dp, cent).start()

        @pl.when(lax.rem(i, upc) == 0)
        def _():
            slot = d * units + i // upc
            remote(
                cnt.at[slot], cnt_dst.at[slot], cnt_send.at[d], cnt_got.at[slot], dp, cent
            ).start()

    def take(d, i, dst, got, cnt_dst, cnt_got):
        at = dst.at[crows(d, i)]
        remote(at, at, sum_send.at[d], got.at[d * count + i], other, cent).wait_recv()

        @pl.when(lax.rem(i, upc) == 0)
        def _():
            slot = d * units + i // upc
            remote(
                cnt_dst.at[slot], cnt_dst.at[slot], cnt_send.at[d], cnt_got.at[slot], other, cent
            ).wait_recv()

    def add(d, i, dst, src, cnt_dst, cnt_src):
        at = crows(d, i)
        dst[at, :] = dst[at, :] + src[at, :]

        @pl.when(lax.rem(i, upc) == 0)
        def _():
            slot = d * units + i // upc
            cnt_dst[slot] = cnt_dst[slot] + cnt_src[slot]

    def result_up(d, i):
        at = out_ref.at[orows(d, i)]
        remote(at, at, up_send.at[d], res_recv.at[d * count + i], me + 2, cent).start()

    def result_down(d, i):
        at = out_ref.at[orows(d, i)]
        remote(at, at, down_send.at[d], res_recv.at[d * count + i], me - 2, cent).start()

    def hand_over(d, i):
        at = out_ref.at[orows(d, i)]
        remote(at, at, xp_send.at[d], xp_recv.at[d], other, cent).start()

    def root_of(d):
        return root0 + d * (root1 - root0)

    def reduce_step(t, d):
        end = root_of(d)
        pos = jnp.where(z < end, z, jnp.where(z > end, last - z, root1))
        i = t - LAG * pos
        ok = (i >= 0) & (i < count)

        @pl.when(ok & (z < end))
        def _():
            @pl.when(z == 0)
            def _():
                pass_on(d, i, part, low, low_recv, cnt_part, cnt_low, cl_recv, me + 2)

            @pl.when(z > 0)
            def _():
                take(d, i, low, low_recv, cnt_low, cl_recv)
                add(d, i, low, part, cnt_low, cnt_part)
                pass_on(d, i, low, low, low_recv, cnt_low, cnt_low, cl_recv, me + 2)

        @pl.when(ok & (z > end))
        def _():
            @pl.when(z == last)
            def _():
                pass_on(d, i, part, high, high_recv, cnt_part, cnt_high, ch_recv, me - 2)

            @pl.when(z < last)
            def _():
                take(d, i, high, high_recv, cnt_high, ch_recv)
                add(d, i, high, part, cnt_high, cnt_part)
                pass_on(d, i, high, high, high_recv, cnt_high, cnt_high, ch_recv, me - 2)

        @pl.when(ok & (z == end))
        def _():
            @pl.when(z > 0)
            def _():
                take(d, i, low, low_recv, cnt_low, cl_recv)
                add(d, i, part, low, cnt_part, cnt_low)

            @pl.when(z < last)
            def _():
                take(d, i, high, high_recv, cnt_high, ch_recv)
                add(d, i, part, high, cnt_part, cnt_high)

            @pl.when(lax.rem(i, upc) == 0)
            def _():
                line = cnt_part[d * units + i // upc] + 1.0
                for h in range(mb // LANES):
                    cnt_col[d, h * LANES:(h + 1) * LANES, :] = jnp.broadcast_to(
                        line[h:h + 1, :], (LANES, LANES)
                    ).T

            at = crows(d, i)
            div = cnt_col[d, pl.ds(pl.multiple_of(lax.rem(i, upc) * chunk, chunk), chunk), :]
            div = jnp.concatenate([div] * (width // LANES), axis=1)
            out_ref[orows(d, i), :] = (part[at, :] + cenf[at, :]) / div

            @pl.when(z > 0)
            def _():
                result_down(d, i)

            @pl.when(z < last)
            def _():
                result_up(d, i)

            hand_over(d, i)

    def result_step(t, d):
        end = root_of(d)
        away = jnp.abs(z - end)
        i = t - LAG * root1 - BACK * away

        @pl.when((away > 0) & (i >= 0) & (i < count))
        def _():
            at = out_ref.at[orows(d, i)]
            remote(at, at, up_send.at[d], res_recv.at[d * count + i], other, cent).wait_recv()

            @pl.when((z < end) & (z > 0))
            def _():
                result_down(d, i)

            @pl.when((z > end) & (z < last))
            def _():
                result_up(d, i)

            hand_over(d, i)

    def tick(t, carry):
        lax.fori_loop(0, 2, lambda s, c: (reduce_step(t, lax.rem(s + flip, 2)), c)[1], 0)
        lax.fori_loop(0, 2, lambda s, c: (result_step(t, lax.rem(s + flip, 2)), c)[1], 0)
        return carry

    def mixed(u, carry):
        lax.fori_loop(u * EVERY, u * EVERY + EVERY, tick, 0)
        weigh(lax.rem(u + flip, 2), 1 + u // 2, 0, nblk)
        return carry

    busy = 2 * (units - 1)
    lax.fori_loop(0, busy, mixed, 0)
    lax.fori_loop(busy * EVERY, count + LAG * root1 + BACK * root1, tick, 0)

    for copy in stat_copies(0) + stat_copies(1):
        copy.wait_send()
    own = pbuf.at[owned(cent)]
    remote(own, own, px_send, pt_recv.at[0], other, cent).wait_send()
    for i in range(ny - 1):
        remote(own, own, py_send.at[i], pt_recv.at[0], other, cent).wait_send()
    for i in range(ny):
        remote(own, own, pc_send.at[i], pt_recv.at[0], other, cent).wait_send()

    for d in (0, 1):
        end = root_of(d)
        at = part.at[pl.ds(d * dirs, dirs)]
        cs = cnt_part.at[pl.ds(d * units, units)]

        @pl.when(z != end)
        def _():
            remote(at, at, sum_send.at[d], low_recv.at[0], other, cent).wait_send()
            remote(cs, cs, cnt_send.at[d], cl_recv.at[0], other, cent).wait_send()

        @pl.when((z <= end) & (z > 0))
        def _():
            remote(at, at, down_send.at[d], res_recv.at[0], other, cent).wait_send()

        @pl.when((z >= end) & (z < last))
        def _():
            remote(at, at, up_send.at[d], res_recv.at[0], other, cent).wait_send()

        here = out_ref.at[pl.ds(pl.multiple_of(x * half + d * dirs, dirs), dirs)]
        there = out_ref.at[pl.ds(pl.multiple_of((1 - x) * half + d * dirs, dirs), dirs)]
        remote(here, there, xp_send.at[d], xp_recv.at[d], other, cent).wait()


def body(ndp, ncent, points, centroids):
    rows, width = points.shape
    half = centroids.shape[0] // 2
    share = rows // ncent
    pb = min(256, share)
    sub = min(32, pb // ncent)
    kb, mb, chunk = 512, 256, 16
    dirs = half // 2
    count = dirs // chunk
    units = dirs // mb
    nblk = rows // pb
    nsub = share // sub
    ny = ncent // 2
    hp = pb // LANES
    f32, bf16 = jnp.float32, jnp.bfloat16
    dma = pltpu.SemaphoreType.DMA
    return pl.pallas_call(
        functools.partial(kernel, ndp, ncent, (rows, half, pb, sub, kb, mb, chunk)),
        out_shape=pltpu.VMEM(centroids.shape, f32),
        in_specs=[pl.BlockSpec(memory_space=pl.ANY)] * 2,
        out_specs=pl.BlockSpec(memory_space=pltpu.VMEM),
        scratch_shapes=[
            pltpu.VMEM((2 * rows, width), f32),
            pltpu.VMEM((2 * rows, width), bf16),
            pltpu.VMEM((half, width), f32),
            pltpu.VMEM((half, width), bf16),
            pltpu.VMEM((half, LANES), f32),
            pltpu.VMEM((half, pb), f32),
            pltpu.VMEM((half, 2 * rows), bf16),
            pltpu.VMEM((2 * ncent, nblk, 4 * hp, LANES), f32),
            pltpu.VMEM((nblk, 2 * hp, LANES), f32),
            pltpu.VMEM((half, width), f32),
            pltpu.VMEM((half, width), f32),
            pltpu.VMEM((half, width), f32),
            pltpu.VMEM((2 * units, 8, LANES), f32),
            pltpu.VMEM((2 * units, 8, LANES), f32),
            pltpu.VMEM((2 * units, 8, LANES), f32),
            pltpu.VMEM((2, mb, LANES), f32),
            dma((ncent + 1,)),
            dma((ncent * nsub,)),
            dma,
            dma((ny - 1,)),
            dma((ny,)),
            dma((4 * ncent,)),
            dma((4 * ncent,)),
            dma((2,)),
            dma((2 * count,)),
            dma((2 * count,)),
            dma((2,)),
            dma((2 * units,)),
            dma((2 * units,)),
            dma((2,)),
            dma((2,)),
            dma((2 * count,)),
            dma((2,)),
            dma((2,)),
        ],
        compiler_params=pltpu.CompilerParams(
            collective_id=0, has_side_effects=True, vmem_limit_bytes=55 * 2**20
        ),
        name="kmeans",
    )(points, centroids)


def solution(mesh):
    placed = (P("dp", None), P("cent", None))
    return jax.shard_map(
        functools.partial(body, mesh.shape["dp"], mesh.shape["cent"]),
        mesh=mesh, in_specs=placed, out_specs=P("cent", None), check_vma=False,
    )
```

```python
import functools

import jax
import jax.numpy as jnp
from jax import lax
from jax.experimental import pallas as pl
from jax.experimental.pallas import tpu as pltpu
from jax.sharding import PartitionSpec as P

MESH = pl.DeviceIdType.MESH
LANES = 128
LAG = 3
BACK = 3
EVERY = 2
LATE = 2
EXTRA = 1
LOG2E = 1.4426950408889634


def kernel(
    ndp, ncent, geo, pts_ref, cen_ref, out_ref,
    pbuf, ph, cenf, cenh, bias, ybuf, expo, stats, scale_ref,
    part, low, high, cnt_part, cnt_low, cnt_high, cnt_col,
    load_sem, pt_recv, px_send, py_send, pc_send, st_send, st_recv,
    sum_send, low_recv, high_recv, cnt_send, cl_recv, ch_recv,
    up_send, down_send, res_recv, xp_send, xp_recv,
):
    rows, half, pb, sub, kb, mb, chunk = geo
    width = pts_ref.shape[1]
    chain = ndp // 2
    last = chain - 1
    root0, root1 = last // 2, last - last // 2
    dirs = half // 2
    count = dirs // chunk
    share = rows // ncent
    seg = pb // ncent
    per = seg // sub
    nsub = share // sub
    nblk = rows // pb
    hp = pb // LANES
    first = nblk - LATE
    upc = mb // chunk
    units = dirs // mb
    ring = (LAG + BACK) * root1 + 4

    me = lax.axis_index("dp")
    cent = lax.axis_index("cent")
    z, x = me // 2, lax.rem(me, 2)
    core, yy = lax.rem(cent, 2), cent // 2
    other = z * 2 + (1 - x)
    mate = yy * 2 + (1 - core)
    mine = x * ncent + cent
    group = 2 * ncent
    ny = ncent // 2
    same = [lax.rem(yy + d, ny) * 2 + core for d in range(1, ny)]
    cross = [lax.rem(yy + d, ny) * 2 + (1 - core) for d in range(1, ny)]

    def remote(src, dst, send, got, dp, ce):
        return pltpu.make_async_remote_copy(
            src_ref=src, dst_ref=dst, send_sem=send, recv_sem=got,
            device_id=(dp, ce), device_id_type=MESH,
        )

    def owned(owner):
        return pl.ds(pl.multiple_of(owner * share, share), share)

    loads = []
    for o in range(ncent):
        owner = lax.rem(cent + o, ncent)
        loads.append(
            pltpu.make_async_copy(pts_ref.at[owned(owner)], pbuf.at[owned(owner)], load_sem.at[o])
        )
    load_c = pltpu.make_async_copy(
        cen_ref.at[pl.ds(pl.multiple_of(x * half, half), half)], cenf, load_sem.at[ncent]
    )
    for copy in loads:
        copy.start()
    load_c.start()

    barrier = pltpu.get_barrier_semaphore()
    for o in range(1, group):
        peer = lax.rem(mine + o, group)
        pl.semaphore_signal(
            barrier, inc=1, device_id=(z * 2 + peer // ncent, lax.rem(peer, ncent)),
            device_id_type=MESH,
        )

    @pl.when(z > 0)
    def _():
        pl.semaphore_signal(barrier, inc=1, device_id=(me - 2, cent), device_id_type=MESH)

    @pl.when(z < last)
    def _():
        pl.semaphore_signal(barrier, inc=1, device_id=(me + 2, cent), device_id_type=MESH)

    ends = jnp.where(z > 0, 1, 0) + jnp.where(z < last, 1, 0)
    pl.semaphore_wait(barrier, group - 1 + ends)
    loads[0].wait()

    def span(side, owner, j):
        return pl.ds(pl.multiple_of(side * rows + owner * share + j * sub, sub), sub)

    for j in range(nsub):
        remote(
            pbuf.at[span(0, cent, j)], pbuf.at[span(1, cent, j)],
            px_send, pt_recv.at[cent * nsub + j], other, cent,
        ).start()
    for copy in loads[1:]:
        copy.wait()
    for d in same:
        for j in range(nsub - EXTRA, nsub):
            remote(
                pbuf.at[span(0, d, j)], pbuf.at[span(1, d, j)],
                px_send, pt_recv.at[d * nsub + j], other, cent,
            ).start()
    load_c.wait()

    root = jnp.float32(1.0) / jnp.sqrt(jnp.float32(width))
    gain = 2.0 * root * LOG2E
    norm_gain = root * LOG2E

    def prepare(k, carry):
        at = pl.ds(pl.multiple_of(k * mb, mb), mb)
        c = cenf[at, :]
        cenh[at, :] = c.astype(jnp.bfloat16)
        bias[at, :] = jnp.broadcast_to(
            jnp.sum(c * c, axis=1, keepdims=True) * norm_gain, (mb, LANES)
        )
        return carry

    lax.fori_loop(0, half // mb, prepare, 0)

    def block(side, b):
        pv = jnp.concatenate([
            pbuf[pl.ds(pl.multiple_of(side * rows + o * share + b * seg, seg), seg), :]
            for o in range(ncent)
        ], axis=0).astype(jnp.bfloat16)
        origin = lax.rem(x + side, 2)
        cols = pl.ds(pl.multiple_of(b * 2 * pb + origin * pb, pb), pb)
        ph[cols, :] = pv

        def logits(k, top):
            at = pl.ds(pl.multiple_of(k * kb, kb), kb)
            inner = lax.dot_general(
                cenh[at, :], pv, (((1,), (1,)), ((), ())), preferred_element_type=jnp.float32
            )
            v = bias[at, :]
            y = inner * gain - jnp.concatenate([v] * hp, axis=1)
            ybuf[at, :] = y
            return jnp.maximum(top, jnp.max(y, axis=0, keepdims=True))

        top = lax.fori_loop(
            0, half // kb, logits, jnp.full((1, pb), -jnp.inf, jnp.float32), unroll=True
        )

        def powers(k, total):
            at = pl.ds(pl.multiple_of(k * kb, kb), kb)
            e = jnp.exp2(ybuf[at, :] - top)
            expo[at, cols] = e.astype(jnp.bfloat16)
            return total + jnp.sum(e, axis=0, keepdims=True)

        total = lax.fori_loop(0, half // kb, powers, jnp.zeros((1, pb), jnp.float32), unroll=True)
        for h in range(hp):
            lane = slice(h * LANES, (h + 1) * LANES)
            stats[mine, b, pl.ds(origin * hp + h, 1), :] = top[:, lane]
            stats[mine, b, pl.ds((2 + origin) * hp + h, 1), :] = total[:, lane]

    def arrived(owner, j):
        at = pbuf.at[span(1, owner, j)]
        remote(at, at, px_send, pt_recv.at[owner * nsub + j], other, cent).wait_recv()

    def forward(owner, j, ce, sem):
        at = pbuf.at[span(1, owner, j)]
        remote(at, at, sem, pt_recv.at[owner * nsub + j], me, ce).start()

    behind = 3

    def relay(s, carry):
        @pl.when(s < nsub)
        def _():
            arrived(cent, s)

            @pl.when(s < nsub - EXTRA)
            def _():
                for i, d in enumerate(same):
                    forward(cent, s, d, py_send.at[i])

            forward(cent, s, mate, pc_send.at[0])

        @pl.when(s >= behind)
        def _():
            for i, d in enumerate(same):
                arrived(d, s - behind)
                forward(d, s - behind, mate, pc_send.at[i + 1])

        return carry

    def relayed(k):
        q = k - nblk + 1
        far = jnp.maximum(nblk + q, per * (q + 1) + behind + 1)
        return jnp.minimum(nsub + behind, jnp.where(q > 0, far, k + 1))

    def stat_copies(late):
        part_of = pl.ds(first, LATE) if late else pl.ds(0, first)
        copies = []
        for o in range(1, group):
            peer = lax.rem(mine + o, group)
            at = stats.at[mine, part_of]
            copies.append(remote(
                at, at, st_send.at[late], st_recv.at[late * group + mine],
                z * 2 + peer // ncent, lax.rem(peer, ncent),
            ))
        return copies

    def stat_wait(late):
        part_of = pl.ds(first, LATE) if late else pl.ds(0, first)
        for o in range(1, group):
            peer = lax.rem(mine + o, group)
            at = stats.at[peer, part_of]
            remote(
                at, at, st_send.at[late], st_recv.at[late * group + peer], other, cent
            ).wait_recv()

    def step(k, carry):
        side, b = k // nblk, lax.rem(k, nblk)

        @pl.when(side > 0)
        def _():
            def ready(j, c):
                arrived(mate, j)
                for d in cross:
                    arrived(d, j)
                return c

            lax.fori_loop(b * per, b * per + per, ready, 0)

        block(side, b)
        begin = relayed(k - 1)
        middle = jnp.minimum(begin + 1, relayed(k))
        lax.fori_loop(begin, middle, relay, 0)

        @pl.when(k == nblk + first - 1)
        def _():
            for copy in stat_copies(0):
                copy.start()

        lax.fori_loop(middle, relayed(k), relay, 0)
        return carry

    lax.fori_loop(0, 2 * nblk, step, 0)
    for copy in stat_copies(1):
        copy.start()

    def settle(late):
        lo, hi = (first, nblk) if late else (0, first)
        stat_wait(late)
        peak = stats[0, lo:hi, 0:2 * hp, :]
        for s in range(1, group):
            peak = jnp.maximum(peak, stats[s, lo:hi, 0:2 * hp, :])
        summed = jnp.zeros((hi - lo, 2 * hp, LANES), jnp.float32)
        for s in range(group):
            summed = summed + stats[s, lo:hi, 2 * hp:, :] * jnp.exp2(stats[s, lo:hi, 0:2 * hp, :] - peak)
        scale_ref[lo:hi] = jnp.exp2(stats[mine, lo:hi, 0:2 * hp, :] - peak) / summed

    def weigh(d, j, lo, hi):
        at = pl.ds(pl.multiple_of(d * dirs + j * mb, mb), mb)
        slot = d * units + j

        def rescale(q, acc):
            cols = pl.ds(pl.multiple_of(q * LANES, LANES), LANES)
            r = expo[at, cols].astype(jnp.float32) * scale_ref[q // (2 * hp), pl.ds(lax.rem(q, 2 * hp), 1), :]
            r = r.astype(jnp.bfloat16)
            expo[at, cols] = r
            return acc + r.astype(jnp.float32)

        scale = 2 * hp
        acc = lax.fori_loop(
            lo * scale, hi * scale, rescale, jnp.zeros((mb, LANES), jnp.float32), unroll=True
        )
        lines = [
            jnp.sum(acc[h * LANES:(h + 1) * LANES, :].T, axis=0, keepdims=True)
            for h in range(mb // LANES)
        ]
        lines = jnp.concatenate(lines * (8 // len(lines)), axis=0)
        pts = slice(lo * 2 * pb, hi * 2 * pb)
        dots = jnp.dot(expo[at, pts], ph[pts, :], preferred_element_type=jnp.float32)
        if lo == 0:
            cnt_part[slot] = lines
            part[at, :] = dots
        else:
            cnt_part[slot] = cnt_part[slot] + lines
            part[at, :] = part[at, :] + dots

    settle(0)
    lax.fori_loop(0, 2, lambda d, c: (weigh(d, 0, 0, first), c)[1], 0)
    settle(1)

    tip = (z == 0) | (z == last)
    flip = jnp.where(z < chain // 2, jnp.where(tip, 1, 0), jnp.where(tip, 0, 1))

    def crows(d, i):
        return pl.ds(pl.multiple_of(d * dirs + i * chunk, chunk), chunk)

    def orows(d, i):
        return pl.ds(pl.multiple_of(x * half + d * dirs + i * chunk, chunk), chunk)

    def pass_on(d, i, src, dst, got, cnt, cnt_dst, cnt_got, dp):
        at = crows(d, i)
        remote(src.at[at], dst.at[at], sum_send.at[d], got.at[d * ring + lax.rem(i, ring)], dp, cent).start()

        @pl.when(lax.rem(i, upc) == 0)
        def _():
            slot = d * units + i // upc
            remote(
                cnt.at[slot], cnt_dst.at[slot], cnt_send.at[d], cnt_got.at[slot], dp, cent
            ).start()

    def take(d, i, dst, got, cnt_dst, cnt_got):
        at = dst.at[crows(d, i)]
        remote(at, at, sum_send.at[d], got.at[d * ring + lax.rem(i, ring)], other, cent).wait_recv()

        @pl.when(lax.rem(i, upc) == 0)
        def _():
            slot = d * units + i // upc
            remote(
                cnt_dst.at[slot], cnt_dst.at[slot], cnt_send.at[d], cnt_got.at[slot], other, cent
            ).wait_recv()

    def add(d, i, dst, src, cnt_dst, cnt_src):
        at = crows(d, i)
        dst[at, :] = dst[at, :] + src[at, :]

        @pl.when(lax.rem(i, upc) == 0)
        def _():
            slot = d * units + i // upc
            cnt_dst[slot] = cnt_dst[slot] + cnt_src[slot]

    def result_up(d, i):
        at = out_ref.at[orows(d, i)]
        remote(at, at, up_send.at[d], res_recv.at[d * ring + lax.rem(i, ring)], me + 2, cent).start()

    def result_down(d, i):
        at = out_ref.at[orows(d, i)]
        remote(at, at, down_send.at[d], res_recv.at[d * ring + lax.rem(i, ring)], me - 2, cent).start()

    def hand_over(d, i):
        at = out_ref.at[orows(d, i)]
        remote(at, at, xp_send.at[d], xp_recv.at[d], other, cent).start()

    def root_of(d):
        return root0 + d * (root1 - root0)

    def reduce_step(t, d):
        end = root_of(d)
        pos = jnp.where(z < end, z, jnp.where(z > end, last - z, root1))
        i = t - LAG * pos
        ok = (i >= 0) & (i < count)

        @pl.when(ok & (z < end))
        def _():
            @pl.when(z == 0)
            def _():
                pass_on(d, i, part, low, low_recv, cnt_part, cnt_low, cl_recv, me + 2)

            @pl.when(z > 0)
            def _():
                take(d, i, low, low_recv, cnt_low, cl_recv)
                add(d, i, low, part, cnt_low, cnt_part)
                pass_on(d, i, low, low, low_recv, cnt_low, cnt_low, cl_recv, me + 2)

        @pl.when(ok & (z > end))
        def _():
            @pl.when(z == last)
            def _():
                pass_on(d, i, part, high, high_recv, cnt_part, cnt_high, ch_recv, me - 2)

            @pl.when(z < last)
            def _():
                take(d, i, high, high_recv, cnt_high, ch_recv)
                add(d, i, high, part, cnt_high, cnt_part)
                pass_on(d, i, high, high, high_recv, cnt_high, cnt_high, ch_recv, me - 2)

        @pl.when(ok & (z == end))
        def _():
            @pl.when(z > 0)
            def _():
                take(d, i, low, low_recv, cnt_low, cl_recv)
                add(d, i, part, low, cnt_part, cnt_low)

            @pl.when(z < last)
            def _():
                take(d, i, high, high_recv, cnt_high, ch_recv)
                add(d, i, part, high, cnt_part, cnt_high)

            @pl.when(lax.rem(i, upc) == 0)
            def _():
                line = cnt_part[d * units + i // upc] + 1.0
                for h in range(mb // LANES):
                    cnt_col[d, h * LANES:(h + 1) * LANES, :] = jnp.broadcast_to(
                        line[h:h + 1, :], (LANES, LANES)
                    ).T

            at = crows(d, i)
            div = cnt_col[d, pl.ds(pl.multiple_of(lax.rem(i, upc) * chunk, chunk), chunk), :]
            div = jnp.concatenate([div] * (width // LANES), axis=1)
            out_ref[orows(d, i), :] = (part[at, :] + cenf[at, :]) / div

            @pl.when(z > 0)
            def _():
                result_down(d, i)

            @pl.when(z < last)
            def _():
                result_up(d, i)

            hand_over(d, i)

    def result_step(t, d):
        end = root_of(d)
        away = jnp.abs(z - end)
        i = t - LAG * root1 - BACK * away

        @pl.when((away > 0) & (i >= 0) & (i < count))
        def _():
            at = out_ref.at[orows(d, i)]
            remote(at, at, up_send.at[d], res_recv.at[d * ring + lax.rem(i, ring)], other, cent).wait_recv()

            @pl.when((z < end) & (z > 0))
            def _():
                result_down(d, i)

            @pl.when((z > end) & (z < last))
            def _():
                result_up(d, i)

            hand_over(d, i)

    def tick(t, carry):
        lax.fori_loop(0, 2, lambda s, c: (result_step(t, lax.rem(s + flip, 2)), c)[1], 0)
        lax.fori_loop(0, 2, lambda s, c: (reduce_step(t, lax.rem(s + flip, 2)), c)[1], 0)
        return carry

    def opening(s, carry):
        d = lax.rem(s + flip, 2)
        weigh(d, 0, first, nblk)
        reduce_step(0, d)
        return carry

    lax.fori_loop(0, 2, opening, 0)

    def mixed(u, carry):
        lax.fori_loop(u * EVERY + 1, u * EVERY + EVERY + 1, tick, 0)
        weigh(lax.rem(u + flip, 2), 1 + u // 2, 0, nblk)
        return carry

    busy = 2 * (units - 1)
    lax.fori_loop(0, busy, mixed, 0)
    lax.fori_loop(busy * EVERY + 1, count + LAG * root1 + BACK * root1, tick, 0)

    def sent(at, sem):
        remote(at, at, sem, pt_recv.at[0], other, cent).wait_send()

    sent(stats.at[pl.ds(0, group - 1), pl.ds(0, first)], st_send.at[0])
    sent(stats.at[pl.ds(0, group - 1), pl.ds(0, LATE)], st_send.at[1])
    sent(pbuf.at[pl.ds(0, share + (ny - 1) * EXTRA * sub)], px_send)
    for i in range(ny - 1):
        sent(pbuf.at[pl.ds(0, share - EXTRA * sub)], py_send.at[i])
    for i in range(ny):
        sent(pbuf.at[pl.ds(0, share)], pc_send.at[i])

    for d in (0, 1):
        end = root_of(d)
        at = part.at[pl.ds(d * dirs, dirs)]
        cs = cnt_part.at[pl.ds(d * units, units)]

        @pl.when(z != end)
        def _():
            remote(at, at, sum_send.at[d], low_recv.at[0], other, cent).wait_send()
            remote(cs, cs, cnt_send.at[d], cl_recv.at[0], other, cent).wait_send()

        @pl.when((z <= end) & (z > 0))
        def _():
            remote(at, at, down_send.at[d], res_recv.at[0], other, cent).wait_send()

        @pl.when((z >= end) & (z < last))
        def _():
            remote(at, at, up_send.at[d], res_recv.at[0], other, cent).wait_send()

        here = out_ref.at[pl.ds(pl.multiple_of(x * half + d * dirs, dirs), dirs)]
        there = out_ref.at[pl.ds(pl.multiple_of((1 - x) * half + d * dirs, dirs), dirs)]
        remote(here, there, xp_send.at[d], xp_recv.at[d], other, cent).wait()


def body(ndp, ncent, points, centroids):
    rows, width = points.shape
    half = centroids.shape[0] // 2
    share = rows // ncent
    pb = min(256, share)
    sub = min(32, pb // ncent)
    kb, mb, chunk = 512, 256, 16
    dirs = half // 2
    units = dirs // mb
    outer = ndp // 2 - 1
    ring = (LAG + BACK) * (outer - outer // 2) + 4
    nblk = rows // pb
    nsub = share // sub
    ny = ncent // 2
    hp = pb // LANES
    f32, bf16 = jnp.float32, jnp.bfloat16
    dma = pltpu.SemaphoreType.DMA
    return pl.pallas_call(
        functools.partial(kernel, ndp, ncent, (rows, half, pb, sub, kb, mb, chunk)),
        out_shape=pltpu.VMEM(centroids.shape, f32),
        in_specs=[pl.BlockSpec(memory_space=pl.ANY)] * 2,
        out_specs=pl.BlockSpec(memory_space=pltpu.VMEM),
        scratch_shapes=[
            pltpu.VMEM((2 * rows, width), f32),
            pltpu.VMEM((2 * rows, width), bf16),
            pltpu.VMEM((half, width), f32),
            pltpu.VMEM((half, width), bf16),
            pltpu.VMEM((half, LANES), f32),
            pltpu.VMEM((half, pb), f32),
            pltpu.VMEM((half, 2 * rows), bf16),
            pltpu.VMEM((2 * ncent, nblk, 4 * hp, LANES), f32),
            pltpu.VMEM((nblk, 2 * hp, LANES), f32),
            pltpu.VMEM((half, width), f32),
            pltpu.VMEM((half, width), f32),
            pltpu.VMEM((half, width), f32),
            pltpu.VMEM((2 * units, 8, LANES), f32),
            pltpu.VMEM((2 * units, 8, LANES), f32),
            pltpu.VMEM((2 * units, 8, LANES), f32),
            pltpu.VMEM((2, mb, LANES), f32),
            dma((ncent + 1,)),
            dma((ncent * nsub,)),
            dma,
            dma((ny - 1,)),
            dma((ny,)),
            dma((2,)),
            dma((4 * ncent,)),
            dma((2,)),
            dma((2 * ring,)),
            dma((2 * ring,)),
            dma((2,)),
            dma((2 * units,)),
            dma((2 * units,)),
            dma((2,)),
            dma((2,)),
            dma((2 * ring,)),
            dma((2,)),
            dma((2,)),
        ],
        compiler_params=pltpu.CompilerParams(
            collective_id=0, has_side_effects=True, vmem_limit_bytes=55 * 2**20
        ),
        name="kmeans",
    )(points, centroids)


def solution(mesh):
    placed = (P("dp", None), P("cent", None))
    return jax.shard_map(
        functools.partial(body, mesh.shape["dp"], mesh.shape["cent"]),
        mesh=mesh, in_specs=placed, out_specs=P("cent", None), check_vma=False,
    )
```

```python
import functools

import jax
import jax.numpy as jnp
from jax import lax
from jax.experimental import pallas as pl
from jax.experimental.pallas import tpu as pltpu
from jax.sharding import PartitionSpec as P

MESH = pl.DeviceIdType.MESH
LANES = 128
LAG = 2
NEXT = 1
BACK = 2
EVERY = 1
BURST = 2
LATE = 2
EXTRA = 1
LOG2E = 1.4426950408889634


def kernel(
    ndp, ncent, geo, pts_ref, cen_ref, out_ref,
    pbuf, ph, cenf, cenh, bias, ybuf, expo, stats, scale_ref,
    part, low, high, cnt_part, cnt_low, cnt_high, cnt_col,
    load_sem, pt_recv, px_send, py_send, pc_send, st_send, st_recv,
    sum_send, low_recv, high_recv, cnt_send, cl_recv, ch_recv,
    up_send, down_send, res_recv, xp_send, xp_recv,
):
    rows, half, pb, sub, kb, mb, chunk = geo
    width = pts_ref.shape[1]
    chain = ndp // 2
    last = chain - 1
    root0, root1 = last // 2, last - last // 2
    dirs = half // 2
    count = dirs // chunk
    share = rows // ncent
    seg = pb // ncent
    per = seg // sub
    nsub = share // sub
    nblk = rows // pb
    hp = pb // LANES
    first = nblk - LATE
    upc = mb // chunk
    units = dirs // mb
    depth = LAG + NEXT * (root1 - 1)
    ring = (depth + BACK * root1) * BURST + 4

    me = lax.axis_index("dp")
    cent = lax.axis_index("cent")
    z, x = me // 2, lax.rem(me, 2)
    core, yy = lax.rem(cent, 2), cent // 2
    other = z * 2 + (1 - x)
    mate = yy * 2 + (1 - core)
    mine = x * ncent + cent
    group = 2 * ncent
    ny = ncent // 2
    same = [lax.rem(yy + d, ny) * 2 + core for d in range(1, ny)]
    cross = [lax.rem(yy + d, ny) * 2 + (1 - core) for d in range(1, ny)]

    def remote(src, dst, send, got, dp, ce):
        return pltpu.make_async_remote_copy(
            src_ref=src, dst_ref=dst, send_sem=send, recv_sem=got,
            device_id=(dp, ce), device_id_type=MESH,
        )

    def owned(owner):
        return pl.ds(pl.multiple_of(owner * share, share), share)

    loads = []
    for o in range(ncent):
        owner = lax.rem(cent + o, ncent)
        loads.append(
            pltpu.make_async_copy(pts_ref.at[owned(owner)], pbuf.at[owned(owner)], load_sem.at[o])
        )
    load_c = pltpu.make_async_copy(
        cen_ref.at[pl.ds(pl.multiple_of(x * half, half), half)], cenf, load_sem.at[ncent]
    )
    for copy in loads:
        copy.start()
    load_c.start()

    barrier = pltpu.get_barrier_semaphore()
    for o in range(1, group):
        peer = lax.rem(mine + o, group)
        pl.semaphore_signal(
            barrier, inc=1, device_id=(z * 2 + peer // ncent, lax.rem(peer, ncent)),
            device_id_type=MESH,
        )

    @pl.when(z > 0)
    def _():
        pl.semaphore_signal(barrier, inc=1, device_id=(me - 2, cent), device_id_type=MESH)

    @pl.when(z < last)
    def _():
        pl.semaphore_signal(barrier, inc=1, device_id=(me + 2, cent), device_id_type=MESH)

    ends = jnp.where(z > 0, 1, 0) + jnp.where(z < last, 1, 0)
    pl.semaphore_wait(barrier, group - 1 + ends)
    loads[0].wait()

    def span(side, owner, j):
        return pl.ds(pl.multiple_of(side * rows + owner * share + j * sub, sub), sub)

    for j in range(nsub):
        remote(
            pbuf.at[span(0, cent, j)], pbuf.at[span(1, cent, j)],
            px_send, pt_recv.at[cent * nsub + j], other, cent,
        ).start()
    for copy in loads[1:]:
        copy.wait()
    for d in same:
        for j in range(nsub - EXTRA, nsub):
            remote(
                pbuf.at[span(0, d, j)], pbuf.at[span(1, d, j)],
                px_send, pt_recv.at[d * nsub + j], other, cent,
            ).start()
    load_c.wait()

    root = jnp.float32(1.0) / jnp.sqrt(jnp.float32(width))
    gain = 2.0 * root * LOG2E
    norm_gain = root * LOG2E

    def prepare(k, carry):
        at = pl.ds(pl.multiple_of(k * mb, mb), mb)
        c = cenf[at, :]
        cenh[at, :] = c.astype(jnp.bfloat16)
        bias[at, :] = jnp.broadcast_to(
            jnp.sum(c * c, axis=1, keepdims=True) * norm_gain, (mb, LANES)
        )
        return carry

    lax.fori_loop(0, half // mb, prepare, 0)

    def block(side, b):
        pv = jnp.concatenate([
            pbuf[pl.ds(pl.multiple_of(side * rows + o * share + b * seg, seg), seg), :]
            for o in range(ncent)
        ], axis=0).astype(jnp.bfloat16)
        origin = lax.rem(x + side, 2)
        cols = pl.ds(pl.multiple_of(b * 2 * pb + origin * pb, pb), pb)
        ph[cols, :] = pv

        def logits(k, top):
            at = pl.ds(pl.multiple_of(k * kb, kb), kb)
            inner = lax.dot_general(
                cenh[at, :], pv, (((1,), (1,)), ((), ())), preferred_element_type=jnp.float32
            )
            v = bias[at, :]
            y = inner * gain - jnp.concatenate([v] * hp, axis=1)
            ybuf[at, :] = y
            return jnp.maximum(top, jnp.max(y, axis=0, keepdims=True))

        top = lax.fori_loop(
            0, half // kb, logits, jnp.full((1, pb), -jnp.inf, jnp.float32), unroll=True
        )

        def powers(k, total):
            at = pl.ds(pl.multiple_of(k * kb, kb), kb)
            e = jnp.exp2(ybuf[at, :] - top)
            expo[at, cols] = e.astype(jnp.bfloat16)
            return total + jnp.sum(e, axis=0, keepdims=True)

        total = lax.fori_loop(0, half // kb, powers, jnp.zeros((1, pb), jnp.float32), unroll=True)
        for h in range(hp):
            lane = slice(h * LANES, (h + 1) * LANES)
            stats[mine, b, pl.ds(origin * hp + h, 1), :] = top[:, lane]
            stats[mine, b, pl.ds((2 + origin) * hp + h, 1), :] = total[:, lane]

    def arrived(owner, j):
        at = pbuf.at[span(1, owner, j)]
        remote(at, at, px_send, pt_recv.at[owner * nsub + j], other, cent).wait_recv()

    def forward(owner, j, ce, sem):
        at = pbuf.at[span(1, owner, j)]
        remote(at, at, sem, pt_recv.at[owner * nsub + j], me, ce).start()

    behind = 3

    def relay(s, carry):
        @pl.when(s < nsub)
        def _():
            arrived(cent, s)

            @pl.when(s < nsub - EXTRA)
            def _():
                for i, d in enumerate(same):
                    forward(cent, s, d, py_send.at[i])

            forward(cent, s, mate, pc_send.at[0])

        @pl.when(s >= behind)
        def _():
            for i, d in enumerate(same):
                arrived(d, s - behind)
                forward(d, s - behind, mate, pc_send.at[i + 1])

        return carry

    def relayed(k):
        q = k - nblk + 1
        far = jnp.maximum(nblk + q, per * (q + 1) + behind + 1)
        far = jnp.where(far >= nsub + behind - 1, nsub + behind, far)
        return jnp.where(q > 0, far, k + 1)

    def stat_copies(late):
        part_of = pl.ds(first, LATE) if late else pl.ds(0, first)
        copies = []
        for o in range(1, group):
            peer = lax.rem(mine + o, group)
            at = stats.at[mine, part_of]
            copies.append(remote(
                at, at, st_send.at[late], st_recv.at[late * group + mine],
                z * 2 + peer // ncent, lax.rem(peer, ncent),
            ))
        return copies

    def stat_wait(late):
        part_of = pl.ds(first, LATE) if late else pl.ds(0, first)
        for o in range(1, group):
            peer = lax.rem(mine + o, group)
            at = stats.at[peer, part_of]
            remote(
                at, at, st_send.at[late], st_recv.at[late * group + peer], other, cent
            ).wait_recv()

    def step(k, carry):
        side, b = k // nblk, lax.rem(k, nblk)

        @pl.when(side > 0)
        def _():
            def ready(j, c):
                arrived(mate, j)
                for d in cross:
                    arrived(d, j)
                return c

            lax.fori_loop(b * per, b * per + per, ready, 0)

        block(side, b)
        begin = relayed(k - 1)
        middle = jnp.minimum(begin + 1, relayed(k))
        lax.fori_loop(begin, middle, relay, 0)

        @pl.when(k == nblk + first - 1)
        def _():
            for copy in stat_copies(0):
                copy.start()

        lax.fori_loop(middle, relayed(k), relay, 0)
        return carry

    lax.fori_loop(0, 2 * nblk, step, 0)
    for copy in stat_copies(1):
        copy.start()

    def settle(late):
        lo, hi = (first, nblk) if late else (0, first)
        stat_wait(late)
        peak = stats[0, lo:hi, 0:2 * hp, :]
        for s in range(1, group):
            peak = jnp.maximum(peak, stats[s, lo:hi, 0:2 * hp, :])
        summed = jnp.zeros((hi - lo, 2 * hp, LANES), jnp.float32)
        for s in range(group):
            summed = summed + stats[s, lo:hi, 2 * hp:, :] * jnp.exp2(stats[s, lo:hi, 0:2 * hp, :] - peak)
        scale_ref[lo:hi] = jnp.exp2(stats[mine, lo:hi, 0:2 * hp, :] - peak) / summed

    def weigh(d, j, lo, hi):
        at = pl.ds(pl.multiple_of(d * dirs + j * mb, mb), mb)
        slot = d * units + j

        def rescale(q, acc):
            cols = pl.ds(pl.multiple_of(q * LANES, LANES), LANES)
            r = expo[at, cols].astype(jnp.float32) * scale_ref[q // (2 * hp), pl.ds(lax.rem(q, 2 * hp), 1), :]
            r = r.astype(jnp.bfloat16)
            expo[at, cols] = r
            return acc + r.astype(jnp.float32)

        scale = 2 * hp
        acc = lax.fori_loop(
            lo * scale, hi * scale, rescale, jnp.zeros((mb, LANES), jnp.float32), unroll=True
        )
        lines = [
            jnp.sum(acc[h * LANES:(h + 1) * LANES, :].T, axis=0, keepdims=True)
            for h in range(mb // LANES)
        ]
        lines = jnp.concatenate(lines * (8 // len(lines)), axis=0)
        pts = slice(lo * 2 * pb, hi * 2 * pb)
        dots = jnp.dot(expo[at, pts], ph[pts, :], preferred_element_type=jnp.float32)
        if lo == 0:
            cnt_part[slot] = lines
            part[at, :] = dots
        else:
            cnt_part[slot] = cnt_part[slot] + lines
            part[at, :] = part[at, :] + dots

    settle(0)
    lax.fori_loop(0, 2, lambda d, c: (weigh(d, 0, 0, first), c)[1], 0)
    settle(1)

    flip = jnp.where(z < chain // 2, 1, 0)

    def crows(d, i):
        return pl.ds(pl.multiple_of(d * dirs + i * chunk, chunk), chunk)

    def orows(d, i):
        return pl.ds(pl.multiple_of(x * half + d * dirs + i * chunk, chunk), chunk)

    def pass_on(d, i, src, dst, got, cnt, cnt_dst, cnt_got, dp):
        at = crows(d, i)
        remote(src.at[at], dst.at[at], sum_send.at[d], got.at[d * ring + lax.rem(i, ring)], dp, cent).start()

        @pl.when(lax.rem(i, upc) == 0)
        def _():
            slot = d * units + i // upc
            remote(
                cnt.at[slot], cnt_dst.at[slot], cnt_send.at[d], cnt_got.at[slot], dp, cent
            ).start()

    def take(d, i, dst, got, cnt_dst, cnt_got):
        at = dst.at[crows(d, i)]
        remote(at, at, sum_send.at[d], got.at[d * ring + lax.rem(i, ring)], other, cent).wait_recv()

        @pl.when(lax.rem(i, upc) == 0)
        def _():
            slot = d * units + i // upc
            remote(
                cnt_dst.at[slot], cnt_dst.at[slot], cnt_send.at[d], cnt_got.at[slot], other, cent
            ).wait_recv()

    def add(d, i, dst, src, cnt_dst, cnt_src):
        at = crows(d, i)
        dst[at, :] = dst[at, :] + src[at, :]

        @pl.when(lax.rem(i, upc) == 0)
        def _():
            slot = d * units + i // upc
            cnt_dst[slot] = cnt_dst[slot] + cnt_src[slot]

    def result_up(d, i):
        at = out_ref.at[orows(d, i)]
        remote(at, at, up_send.at[d], res_recv.at[d * ring + lax.rem(i, ring)], me + 2, cent).start()

    def result_down(d, i):
        at = out_ref.at[orows(d, i)]
        remote(at, at, down_send.at[d], res_recv.at[d * ring + lax.rem(i, ring)], me - 2, cent).start()

    def hand_over(d, i):
        at = out_ref.at[orows(d, i)]
        remote(at, at, xp_send.at[d], xp_recv.at[d], other, cent).start()

    def root_of(d):
        return root0 + d * (root1 - root0)

    def reduce_step(t, d, c):
        end = root_of(d)
        pos = jnp.where(z < end, z, jnp.where(z > end, last - z, root1))
        i = (t - jnp.where(pos > 0, LAG + NEXT * (pos - 1), 0)) * BURST + c
        ok = (i >= 0) & (i < count)

        @pl.when(ok & (z < end))
        def _():
            @pl.when(z == 0)
            def _():
                pass_on(d, i, part, low, low_recv, cnt_part, cnt_low, cl_recv, me + 2)

            @pl.when(z > 0)
            def _():
                take(d, i, low, low_recv, cnt_low, cl_recv)
                add(d, i, low, part, cnt_low, cnt_part)
                pass_on(d, i, low, low, low_recv, cnt_low, cnt_low, cl_recv, me + 2)

        @pl.when(ok & (z > end))
        def _():
            @pl.when(z == last)
            def _():
                pass_on(d, i, part, high, high_recv, cnt_part, cnt_high, ch_recv, me - 2)

            @pl.when(z < last)
            def _():
                take(d, i, high, high_recv, cnt_high, ch_recv)
                add(d, i, high, part, cnt_high, cnt_part)
                pass_on(d, i, high, high, high_recv, cnt_high, cnt_high, ch_recv, me - 2)

        @pl.when(ok & (z == end))
        def _():
            @pl.when(z > 0)
            def _():
                take(d, i, low, low_recv, cnt_low, cl_recv)
                add(d, i, part, low, cnt_part, cnt_low)

            @pl.when(z < last)
            def _():
                take(d, i, high, high_recv, cnt_high, ch_recv)
                add(d, i, part, high, cnt_part, cnt_high)

            @pl.when(lax.rem(i, upc) == 0)
            def _():
                line = cnt_part[d * units + i // upc] + 1.0
                for h in range(mb // LANES):
                    cnt_col[d, h * LANES:(h + 1) * LANES, :] = jnp.broadcast_to(
                        line[h:h + 1, :], (LANES, LANES)
                    ).T

            at = crows(d, i)
            div = cnt_col[d, pl.ds(pl.multiple_of(lax.rem(i, upc) * chunk, chunk), chunk), :]
            div = jnp.concatenate([div] * (width // LANES), axis=1)
            out_ref[orows(d, i), :] = (part[at, :] + cenf[at, :]) / div

            @pl.when(z > 0)
            def _():
                result_down(d, i)

            @pl.when(z < last)
            def _():
                result_up(d, i)

            hand_over(d, i)

    def result_step(t, d, c):
        end = root_of(d)
        away = jnp.abs(z - end)
        i = (t - depth - BACK * away) * BURST + c

        @pl.when((away > 0) & (i >= 0) & (i < count))
        def _():
            at = out_ref.at[orows(d, i)]
            remote(at, at, up_send.at[d], res_recv.at[d * ring + lax.rem(i, ring)], other, cent).wait_recv()

            @pl.when((z < end) & (z > 0))
            def _():
                result_down(d, i)

            @pl.when((z > end) & (z < last))
            def _():
                result_up(d, i)

            hand_over(d, i)

    def tick(t, carry):
        def back(s, c):
            result_step(t, lax.rem(s // BURST + flip, 2), lax.rem(s, BURST))
            return c

        def out(s, c):
            reduce_step(t, lax.rem(s // BURST + flip, 2), lax.rem(s, BURST))
            return c

        lax.fori_loop(0, 2 * BURST, back, 0)
        lax.fori_loop(0, 2 * BURST, out, 0)
        return carry

    def opening(s, carry):
        d = lax.rem(s + flip, 2)
        weigh(d, 0, first, nblk)
        lax.fori_loop(0, BURST, lambda c, n: (reduce_step(0, d, c), n)[1], 0)
        return carry

    lax.fori_loop(0, 2, opening, 0)

    def mixed(u, carry):
        lax.fori_loop(u * EVERY + 1, u * EVERY + EVERY + 1, tick, 0)
        weigh(lax.rem(u + flip, 2), 1 + u // 2, 0, nblk)
        return carry

    busy = 2 * (units - 1)
    lax.fori_loop(0, busy, mixed, 0)
    lax.fori_loop(busy * EVERY + 1, count // BURST + depth + BACK * root1, tick, 0)

    def sent(at, sem):
        remote(at, at, sem, pt_recv.at[0], other, cent).wait_send()

    sent(stats.at[pl.ds(0, group - 1), pl.ds(0, first)], st_send.at[0])
    sent(stats.at[pl.ds(0, group - 1), pl.ds(0, LATE)], st_send.at[1])
    sent(pbuf.at[pl.ds(0, share + (ny - 1) * EXTRA * sub)], px_send)
    for i in range(ny - 1):
        sent(pbuf.at[pl.ds(0, share - EXTRA * sub)], py_send.at[i])
    for i in range(ny):
        sent(pbuf.at[pl.ds(0, share)], pc_send.at[i])

    for d in (0, 1):
        end = root_of(d)
        at = part.at[pl.ds(d * dirs, dirs)]
        cs = cnt_part.at[pl.ds(d * units, units)]

        @pl.when(z != end)
        def _():
            remote(at, at, sum_send.at[d], low_recv.at[0], other, cent).wait_send()
            remote(cs, cs, cnt_send.at[d], cl_recv.at[0], other, cent).wait_send()

        @pl.when((z <= end) & (z > 0))
        def _():
            remote(at, at, down_send.at[d], res_recv.at[0], other, cent).wait_send()

        @pl.when((z >= end) & (z < last))
        def _():
            remote(at, at, up_send.at[d], res_recv.at[0], other, cent).wait_send()

        here = out_ref.at[pl.ds(pl.multiple_of(x * half + d * dirs, dirs), dirs)]
        there = out_ref.at[pl.ds(pl.multiple_of((1 - x) * half + d * dirs, dirs), dirs)]
        remote(here, there, xp_send.at[d], xp_recv.at[d], other, cent).wait()


def body(ndp, ncent, points, centroids):
    rows, width = points.shape
    half = centroids.shape[0] // 2
    share = rows // ncent
    pb = min(256, share)
    sub = min(32, pb // ncent)
    kb, mb, chunk = 512, 256, 16
    dirs = half // 2
    units = dirs // mb
    outer = ndp // 2 - 1
    ring = (LAG + NEXT * (outer - outer // 2 - 1) + BACK * (outer - outer // 2)) * BURST + 4
    nblk = rows // pb
    nsub = share // sub
    ny = ncent // 2
    hp = pb // LANES
    f32, bf16 = jnp.float32, jnp.bfloat16
    dma = pltpu.SemaphoreType.DMA
    return pl.pallas_call(
        functools.partial(kernel, ndp, ncent, (rows, half, pb, sub, kb, mb, chunk)),
        out_shape=pltpu.VMEM(centroids.shape, f32),
        in_specs=[pl.BlockSpec(memory_space=pl.ANY)] * 2,
        out_specs=pl.BlockSpec(memory_space=pltpu.VMEM),
        scratch_shapes=[
            pltpu.VMEM((2 * rows, width), f32),
            pltpu.VMEM((2 * rows, width), bf16),
            pltpu.VMEM((half, width), f32),
            pltpu.VMEM((half, width), bf16),
            pltpu.VMEM((half, LANES), f32),
            pltpu.VMEM((half, pb), f32),
            pltpu.VMEM((half, 2 * rows), bf16),
            pltpu.VMEM((2 * ncent, nblk, 4 * hp, LANES), f32),
            pltpu.VMEM((nblk, 2 * hp, LANES), f32),
            pltpu.VMEM((half, width), f32),
            pltpu.VMEM((half, width), f32),
            pltpu.VMEM((half, width), f32),
            pltpu.VMEM((2 * units, 8, LANES), f32),
            pltpu.VMEM((2 * units, 8, LANES), f32),
            pltpu.VMEM((2 * units, 8, LANES), f32),
            pltpu.VMEM((2, mb, LANES), f32),
            dma((ncent + 1,)),
            dma((ncent * nsub,)),
            dma,
            dma((ny - 1,)),
            dma((ny,)),
            dma((2,)),
            dma((4 * ncent,)),
            dma((2,)),
            dma((2 * ring,)),
            dma((2 * ring,)),
            dma((2,)),
            dma((2 * units,)),
            dma((2 * units,)),
            dma((2,)),
            dma((2,)),
            dma((2 * ring,)),
            dma((2,)),
            dma((2,)),
        ],
        compiler_params=pltpu.CompilerParams(
            collective_id=0, has_side_effects=True, vmem_limit_bytes=55 * 2**20
        ),
        name="kmeans",
    )(points, centroids)


def solution(mesh):
    placed = (P("dp", None), P("cent", None))
    return jax.shard_map(
        functools.partial(body, mesh.shape["dp"], mesh.shape["cent"]),
        mesh=mesh, in_specs=placed, out_specs=P("cent", None), check_vma=False,
    )
```

```python
import functools

import jax
import jax.numpy as jnp
from jax import lax
from jax.experimental import pallas as pl
from jax.experimental.pallas import tpu as pltpu
from jax.sharding import PartitionSpec as P

MESH = pl.DeviceIdType.MESH
LANES = 128
LAG = 2
NEXT = 1
BACK = 2
EVERY = 1
BURST = 2
LATE = 2
EXTRA = 1
LOG2E = 1.4426950408889634


def kernel(
    ndp, ncent, geo, pts_ref, cen_ref, out_ref,
    pbuf, ph, cenf, cenh, bias, ybuf, expo, stats, near, scale_ref,
    part, low, high, cnt_part, cnt_low, cnt_high, cnt_col,
    load_sem, pt_recv, px_send, py_send, pc_send, st_send, st_recv,
    sum_send, low_recv, high_recv, cnt_send, cl_recv, ch_recv,
    up_send, down_send, res_recv, xp_send, xp_recv,
):
    rows, half, pb, sub, kb, mb, chunk = geo
    width = pts_ref.shape[1]
    chain = ndp // 2
    last = chain - 1
    root0, root1 = last // 2, last - last // 2
    dirs = half // 2
    count = dirs // chunk
    share = rows // ncent
    seg = pb // ncent
    per = seg // sub
    nsub = share // sub
    nblk = rows // pb
    hp = pb // LANES
    first = nblk - LATE
    upc = mb // chunk
    units = dirs // mb
    depth = LAG + NEXT * (root1 - 1)
    ring = (depth + BACK * root1) * BURST

    me = lax.axis_index("dp")
    cent = lax.axis_index("cent")
    z, x = me // 2, lax.rem(me, 2)
    core, yy = lax.rem(cent, 2), cent // 2
    other = z * 2 + (1 - x)
    mate = yy * 2 + (1 - core)
    mine = x * ncent + cent
    group = 2 * ncent
    ny = ncent // 2
    same = [lax.rem(yy + d, ny) * 2 + core for d in range(1, ny)]
    cross = [lax.rem(yy + d, ny) * 2 + (1 - core) for d in range(1, ny)]

    def remote(src, dst, send, got, dp, ce):
        return pltpu.make_async_remote_copy(
            src_ref=src, dst_ref=dst, send_sem=send, recv_sem=got,
            device_id=(dp, ce), device_id_type=MESH,
        )

    def owned(owner):
        return pl.ds(pl.multiple_of(owner * share, share), share)

    loads = []
    for o in range(ncent):
        owner = lax.rem(cent + o, ncent)
        loads.append(
            pltpu.make_async_copy(pts_ref.at[owned(owner)], pbuf.at[owned(owner)], load_sem.at[o])
        )
    load_c = pltpu.make_async_copy(
        cen_ref.at[pl.ds(pl.multiple_of(x * half, half), half)], cenf, load_sem.at[ncent]
    )
    for copy in loads:
        copy.start()
    load_c.start()

    barrier = pltpu.get_barrier_semaphore()
    for o in range(1, group):
        peer = lax.rem(mine + o, group)
        pl.semaphore_signal(
            barrier, inc=1, device_id=(z * 2 + peer // ncent, lax.rem(peer, ncent)),
            device_id_type=MESH,
        )

    @pl.when(z > 0)
    def _():
        pl.semaphore_signal(barrier, inc=1, device_id=(me - 2, cent), device_id_type=MESH)

    @pl.when(z < last)
    def _():
        pl.semaphore_signal(barrier, inc=1, device_id=(me + 2, cent), device_id_type=MESH)

    ends = jnp.where(z > 0, 1, 0) + jnp.where(z < last, 1, 0)
    pl.semaphore_wait(barrier, group - 1 + ends)
    loads[0].wait()

    def span(side, owner, j):
        return pl.ds(pl.multiple_of(side * rows + owner * share + j * sub, sub), sub)

    for j in range(nsub):
        remote(
            pbuf.at[span(0, cent, j)], pbuf.at[span(1, cent, j)],
            px_send, pt_recv.at[cent * nsub + j], other, cent,
        ).start()
    for copy in loads[1:]:
        copy.wait()
    for d in same:
        for j in range(nsub - EXTRA, nsub):
            remote(
                pbuf.at[span(0, d, j)], pbuf.at[span(1, d, j)],
                px_send, pt_recv.at[d * nsub + j], other, cent,
            ).start()
    load_c.wait()

    root = jnp.float32(1.0) / jnp.sqrt(jnp.float32(width))
    gain = 2.0 * root * LOG2E
    norm_gain = root * LOG2E

    def prepare(k, carry):
        at = pl.ds(pl.multiple_of(k * mb, mb), mb)
        c = cenf[at, :]
        cenh[at, :] = c.astype(jnp.bfloat16)
        bias[at, :] = jnp.broadcast_to(
            jnp.sum(c * c, axis=1, keepdims=True) * norm_gain, (mb, LANES)
        )
        return carry

    lax.fori_loop(0, half // mb, prepare, 0)

    def block(side, b):
        pv = jnp.concatenate([
            pbuf[pl.ds(pl.multiple_of(side * rows + o * share + b * seg, seg), seg), :]
            for o in range(ncent)
        ], axis=0).astype(jnp.bfloat16)
        origin = lax.rem(x + side, 2)
        cols = pl.ds(pl.multiple_of(b * 2 * pb + origin * pb, pb), pb)
        ph[cols, :] = pv

        tops, sums = [], []
        for k in range(half // kb):
            at = slice(k * kb, (k + 1) * kb)
            inner = lax.dot_general(
                cenh[at, :], pv, (((1,), (1,)), ((), ())), preferred_element_type=jnp.float32
            )
            v = bias[at, :]
            y = inner * gain - jnp.concatenate([v] * hp, axis=1)
            ybuf[at, :] = y
            tops.append(jnp.max(y, axis=0, keepdims=True))
            e = jnp.exp2(ybuf[at, :] - tops[k])
            expo[at, cols] = e.astype(jnp.bfloat16)
            sums.append(jnp.sum(e, axis=0, keepdims=True))
        top = functools.reduce(jnp.maximum, tops)
        total = functools.reduce(jnp.add, [n * jnp.exp2(m - top) for m, n in zip(tops, sums)])
        for h in range(hp):
            lane = slice(h * LANES, (h + 1) * LANES)
            for k, m in enumerate(tops):
                near[k, b, pl.ds(origin * hp + h, 1), :] = m[:, lane]
            stats[mine, b, pl.ds(origin * hp + h, 1), :] = top[:, lane]
            stats[mine, b, pl.ds((2 + origin) * hp + h, 1), :] = total[:, lane]

    def arrived(owner, j):
        at = pbuf.at[span(1, owner, j)]
        remote(at, at, px_send, pt_recv.at[owner * nsub + j], other, cent).wait_recv()

    def forward(owner, j, ce, sem):
        at = pbuf.at[span(1, owner, j)]
        remote(at, at, sem, pt_recv.at[owner * nsub + j], me, ce).start()

    behind = 3

    def relay(s, carry):
        @pl.when(s < nsub)
        def _():
            arrived(cent, s)

            @pl.when(s < nsub - EXTRA)
            def _():
                for i, d in enumerate(same):
                    forward(cent, s, d, py_send.at[i])

            forward(cent, s, mate, pc_send.at[0])

        @pl.when(s >= behind)
        def _():
            for i, d in enumerate(same):
                arrived(d, s - behind)
                forward(d, s - behind, mate, pc_send.at[i + 1])

        return carry

    def relayed(k):
        q = k - nblk + 1
        far = jnp.maximum(nblk + q, per * (q + 1) + behind + 1)
        far = jnp.where(far >= nsub + behind - 1, nsub + behind, far)
        return jnp.where(q > 0, far, k + 1)

    def stat_copies(late):
        part_of = pl.ds(first, LATE) if late else pl.ds(0, first)
        copies = []
        for o in range(1, group):
            peer = lax.rem(mine + o, group)
            at = stats.at[mine, part_of]
            copies.append(remote(
                at, at, st_send.at[late], st_recv.at[late * group + mine],
                z * 2 + peer // ncent, lax.rem(peer, ncent),
            ))
        return copies

    def stat_wait(late):
        part_of = pl.ds(first, LATE) if late else pl.ds(0, first)
        for o in range(1, group):
            peer = lax.rem(mine + o, group)
            at = stats.at[peer, part_of]
            remote(
                at, at, st_send.at[late], st_recv.at[late * group + peer], other, cent
            ).wait_recv()

    def step(k, carry):
        side, b = k // nblk, lax.rem(k, nblk)

        @pl.when(side > 0)
        def _():
            def ready(j, c):
                arrived(mate, j)
                for d in cross:
                    arrived(d, j)
                return c

            lax.fori_loop(b * per, b * per + per, ready, 0)

        block(side, b)
        begin = relayed(k - 1)
        middle = jnp.minimum(begin + 1, relayed(k))
        lax.fori_loop(begin, middle, relay, 0)

        @pl.when(k == nblk + first - 1)
        def _():
            for copy in stat_copies(0):
                copy.start()

        lax.fori_loop(middle, relayed(k), relay, 0)
        return carry

    lax.fori_loop(0, 2 * nblk, step, 0)
    for copy in stat_copies(1):
        copy.start()

    def settle(late):
        lo, hi = (first, nblk) if late else (0, first)
        stat_wait(late)
        peak = stats[0, lo:hi, 0:2 * hp, :]
        for s in range(1, group):
            peak = jnp.maximum(peak, stats[s, lo:hi, 0:2 * hp, :])
        summed = jnp.zeros((hi - lo, 2 * hp, LANES), jnp.float32)
        for s in range(group):
            summed = summed + stats[s, lo:hi, 2 * hp:, :] * jnp.exp2(stats[s, lo:hi, 0:2 * hp, :] - peak)
        for k in range(half // kb):
            scale_ref[k, lo:hi] = jnp.exp2(near[k, lo:hi] - peak) / summed

    def weigh(d, j, lo, hi):
        at = pl.ds(pl.multiple_of(d * dirs + j * mb, mb), mb)
        slot = d * units + j
        piece = (d * dirs + j * mb) // kb

        def rescale(q, acc):
            cols = pl.ds(pl.multiple_of(q * LANES, LANES), LANES)
            r = expo[at, cols].astype(jnp.float32) * scale_ref[piece, q // (2 * hp), pl.ds(lax.rem(q, 2 * hp), 1), :]
            r = r.astype(jnp.bfloat16)
            expo[at, cols] = r
            return acc + r.astype(jnp.float32)

        scale = 2 * hp
        acc = lax.fori_loop(
            lo * scale, hi * scale, rescale, jnp.zeros((mb, LANES), jnp.float32), unroll=True
        )
        lines = [
            jnp.sum(acc[h * LANES:(h + 1) * LANES, :].T, axis=0, keepdims=True)
            for h in range(mb // LANES)
        ]
        lines = jnp.concatenate(lines * (8 // len(lines)), axis=0)
        pts = slice(lo * 2 * pb, hi * 2 * pb)
        dots = jnp.dot(expo[at, pts], ph[pts, :], preferred_element_type=jnp.float32)
        if lo == 0:
            cnt_part[slot] = lines
            part[at, :] = dots
        else:
            cnt_part[slot] = cnt_part[slot] + lines
            part[at, :] = part[at, :] + dots

    settle(0)
    lax.fori_loop(0, 2, lambda d, c: (weigh(d, 0, 0, first), c)[1], 0)
    settle(1)

    flip = jnp.where(z < chain // 2, 1, 0)

    def crows(d, i):
        return pl.ds(pl.multiple_of(d * dirs + i * chunk, chunk), chunk)

    def orows(d, i):
        return pl.ds(pl.multiple_of(x * half + d * dirs + i * chunk, chunk), chunk)

    def pass_on(d, i, src, dst, got, cnt, cnt_dst, cnt_got, dp):
        at = crows(d, i)
        remote(src.at[at], dst.at[at], sum_send.at[d], got.at[d * ring + lax.rem(i, ring)], dp, cent).start()

        @pl.when(lax.rem(i, upc) == 0)
        def _():
            slot = d * units + i // upc
            remote(
                cnt.at[slot], cnt_dst.at[slot], cnt_send.at[d], cnt_got.at[d * 2 + lax.rem(i // upc, 2)], dp, cent
            ).start()

    def take(d, i, dst, got, cnt_dst, cnt_got):
        at = dst.at[crows(d, i)]
        remote(at, at, sum_send.at[d], got.at[d * ring + lax.rem(i, ring)], other, cent).wait_recv()

        @pl.when(lax.rem(i, upc) == 0)
        def _():
            slot = d * units + i // upc
            remote(
                cnt_dst.at[slot], cnt_dst.at[slot], cnt_send.at[d], cnt_got.at[d * 2 + lax.rem(i // upc, 2)], other, cent
            ).wait_recv()

    def add(d, i, dst, src, cnt_dst, cnt_src):
        at = crows(d, i)
        dst[at, :] = dst[at, :] + src[at, :]

        @pl.when(lax.rem(i, upc) == 0)
        def _():
            slot = d * units + i // upc
            cnt_dst[slot] = cnt_dst[slot] + cnt_src[slot]

    def result_up(d, i):
        at = out_ref.at[orows(d, i)]
        remote(at, at, up_send.at[d], res_recv.at[d * ring + lax.rem(i, ring)], me + 2, cent).start()

    def result_down(d, i):
        at = out_ref.at[orows(d, i)]
        remote(at, at, down_send.at[d], res_recv.at[d * ring + lax.rem(i, ring)], me - 2, cent).start()

    def hand_over(d, i):
        at = out_ref.at[orows(d, i)]
        remote(at, at, xp_send.at[d], xp_recv.at[d], other, cent).start()

    def root_of(d):
        return root0 + d * (root1 - root0)

    def reduce_step(t, d, c):
        end = root_of(d)
        pos = jnp.where(z < end, z, jnp.where(z > end, last - z, root1))
        i = (t - jnp.where(pos > 0, LAG + NEXT * (pos - 1), 0)) * BURST + c
        ok = (i >= 0) & (i < count)

        @pl.when(ok & (z < end))
        def _():
            @pl.when(z == 0)
            def _():
                pass_on(d, i, part, low, low_recv, cnt_part, cnt_low, cl_recv, me + 2)

            @pl.when(z > 0)
            def _():
                take(d, i, low, low_recv, cnt_low, cl_recv)
                add(d, i, low, part, cnt_low, cnt_part)
                pass_on(d, i, low, low, low_recv, cnt_low, cnt_low, cl_recv, me + 2)

        @pl.when(ok & (z > end))
        def _():
            @pl.when(z == last)
            def _():
                pass_on(d, i, part, high, high_recv, cnt_part, cnt_high, ch_recv, me - 2)

            @pl.when(z < last)
            def _():
                take(d, i, high, high_recv, cnt_high, ch_recv)
                add(d, i, high, part, cnt_high, cnt_part)
                pass_on(d, i, high, high, high_recv, cnt_high, cnt_high, ch_recv, me - 2)

        @pl.when(ok & (z == end))
        def _():
            @pl.when(z > 0)
            def _():
                take(d, i, low, low_recv, cnt_low, cl_recv)
                add(d, i, part, low, cnt_part, cnt_low)

            @pl.when(z < last)
            def _():
                take(d, i, high, high_recv, cnt_high, ch_recv)
                add(d, i, part, high, cnt_part, cnt_high)

            @pl.when(lax.rem(i, upc) == 0)
            def _():
                line = cnt_part[d * units + i // upc] + 1.0
                for h in range(mb // LANES):
                    cnt_col[d, h * LANES:(h + 1) * LANES, :] = jnp.broadcast_to(
                        line[h:h + 1, :], (LANES, LANES)
                    ).T

            at = crows(d, i)
            div = cnt_col[d, pl.ds(pl.multiple_of(lax.rem(i, upc) * chunk, chunk), chunk), :]
            div = jnp.concatenate([div] * (width // LANES), axis=1)
            out_ref[orows(d, i), :] = (part[at, :] + cenf[at, :]) / div

            @pl.when(z > 0)
            def _():
                result_down(d, i)

            @pl.when(z < last)
            def _():
                result_up(d, i)

            hand_over(d, i)

    def result_step(t, d, c):
        end = root_of(d)
        away = jnp.abs(z - end)
        i = (t - depth - BACK * away) * BURST + c

        @pl.when((away > 0) & (i >= 0) & (i < count))
        def _():
            at = out_ref.at[orows(d, i)]
            remote(at, at, up_send.at[d], res_recv.at[d * ring + lax.rem(i, ring)], other, cent).wait_recv()

            @pl.when((z < end) & (z > 0))
            def _():
                result_down(d, i)

            @pl.when((z > end) & (z < last))
            def _():
                result_up(d, i)

            hand_over(d, i)

    def tick(t, carry):
        def back(s, c):
            result_step(t, lax.rem(s // BURST + flip, 2), lax.rem(s, BURST))
            return c

        def out(s, c):
            reduce_step(t, lax.rem(s // BURST + flip, 2), lax.rem(s, BURST))
            return c

        lax.fori_loop(0, 2 * BURST, back, 0)
        lax.fori_loop(0, 2 * BURST, out, 0)
        return carry

    def opening(s, carry):
        d = lax.rem(s + flip, 2)
        weigh(d, 0, first, nblk)
        lax.fori_loop(0, BURST, lambda c, n: (reduce_step(0, d, c), n)[1], 0)
        return carry

    lax.fori_loop(0, 2, opening, 0)

    def mixed(u, carry):
        lax.fori_loop(u * EVERY + 1, u * EVERY + EVERY + 1, tick, 0)
        weigh(lax.rem(u + flip, 2), 1 + u // 2, 0, nblk)
        return carry

    busy = 2 * (units - 1)
    lax.fori_loop(0, busy, mixed, 0)
    lax.fori_loop(busy * EVERY + 1, count // BURST + depth + BACK * root1, tick, 0)

    def sent(at, sem):
        remote(at, at, sem, pt_recv.at[0], other, cent).wait_send()

    sent(stats.at[pl.ds(0, group - 1), pl.ds(0, first)], st_send.at[0])
    sent(stats.at[pl.ds(0, group - 1), pl.ds(0, LATE)], st_send.at[1])
    sent(pbuf.at[pl.ds(0, share + (ny - 1) * EXTRA * sub)], px_send)
    for i in range(ny - 1):
        sent(pbuf.at[pl.ds(0, share - EXTRA * sub)], py_send.at[i])
    for i in range(ny):
        sent(pbuf.at[pl.ds(0, share)], pc_send.at[i])

    for d in (0, 1):
        end = root_of(d)
        at = part.at[pl.ds(d * dirs, dirs)]
        cs = cnt_part.at[pl.ds(d * units, units)]

        @pl.when(z != end)
        def _():
            remote(at, at, sum_send.at[d], low_recv.at[0], other, cent).wait_send()
            remote(cs, cs, cnt_send.at[d], cl_recv.at[0], other, cent).wait_send()

        @pl.when((z <= end) & (z > 0))
        def _():
            remote(at, at, down_send.at[d], res_recv.at[0], other, cent).wait_send()

        @pl.when((z >= end) & (z < last))
        def _():
            remote(at, at, up_send.at[d], res_recv.at[0], other, cent).wait_send()

        here = out_ref.at[pl.ds(pl.multiple_of(x * half + d * dirs, dirs), dirs)]
        there = out_ref.at[pl.ds(pl.multiple_of((1 - x) * half + d * dirs, dirs), dirs)]
        remote(here, there, xp_send.at[d], xp_recv.at[d], other, cent).wait()


def body(ndp, ncent, points, centroids):
    rows, width = points.shape
    half = centroids.shape[0] // 2
    share = rows // ncent
    pb = min(256, share)
    sub = min(32, pb // ncent)
    kb, mb, chunk = 512, 256, 16
    dirs = half // 2
    units = dirs // mb
    outer = ndp // 2 - 1
    ring = (LAG + NEXT * (outer - outer // 2 - 1) + BACK * (outer - outer // 2)) * BURST
    nblk = rows // pb
    nsub = share // sub
    ny = ncent // 2
    hp = pb // LANES
    f32, bf16 = jnp.float32, jnp.bfloat16
    dma = pltpu.SemaphoreType.DMA
    return pl.pallas_call(
        functools.partial(kernel, ndp, ncent, (rows, half, pb, sub, kb, mb, chunk)),
        out_shape=pltpu.VMEM(centroids.shape, f32),
        in_specs=[pl.BlockSpec(memory_space=pl.ANY)] * 2,
        out_specs=pl.BlockSpec(memory_space=pltpu.VMEM),
        scratch_shapes=[
            pltpu.VMEM((2 * rows, width), f32),
            pltpu.VMEM((2 * rows, width), bf16),
            pltpu.VMEM((half, width), f32),
            pltpu.VMEM((half, width), bf16),
            pltpu.VMEM((half, LANES), f32),
            pltpu.VMEM((half, pb), f32),
            pltpu.VMEM((half, 2 * rows), bf16),
            pltpu.VMEM((2 * ncent, nblk, 4 * hp, LANES), f32),
            pltpu.VMEM((half // kb, nblk, 2 * hp, LANES), f32),
            pltpu.VMEM((half // kb, nblk, 2 * hp, LANES), f32),
            pltpu.VMEM((half, width), f32),
            pltpu.VMEM((half, width), f32),
            pltpu.VMEM((half, width), f32),
            pltpu.VMEM((2 * units, 8, LANES), f32),
            pltpu.VMEM((2 * units, 8, LANES), f32),
            pltpu.VMEM((2 * units, 8, LANES), f32),
            pltpu.VMEM((2, mb, LANES), f32),
            dma((ncent + 1,)),
            dma((ncent * nsub,)),
            dma,
            dma((ny - 1,)),
            dma((ny,)),
            dma((2,)),
            dma((4 * ncent,)),
            dma((2,)),
            dma((2 * ring,)),
            dma((2 * ring,)),
            dma((2,)),
            dma((4,)),
            dma((4,)),
            dma((2,)),
            dma((2,)),
            dma((2 * ring,)),
            dma((2,)),
            dma((2,)),
        ],
        compiler_params=pltpu.CompilerParams(
            collective_id=0, has_side_effects=True, vmem_limit_bytes=55 * 2**20
        ),
        name="kmeans",
    )(points, centroids)


def solution(mesh):
    placed = (P("dp", None), P("cent", None))
    return jax.shard_map(
        functools.partial(body, mesh.shape["dp"], mesh.shape["cent"]),
        mesh=mesh, in_specs=placed, out_specs=P("cent", None), check_vma=False,
    )
```
